16 devices in a mesh: data: 2 (over y, z), model: 8 (over x, core).
Axes of the slice: x: 4, y: 2, z: 1, core: 2. Of those that a mesh axis runs over, the one named last changes fastest.
The devices are a block of a 4x4x8 slice.
Arguments:
- hidden_in: bfloat16 [256, 1024], P('data'), parts along dimension 0
- positions: int32 [256], P('data'), parts along dimension 0
- norm_attn: bfloat16 [4, 1024], replicated
- norm_mlp: bfloat16 [4, 1024], replicated
- w_query: bfloat16 [4, 1024, 1024], P(None, None, 'model')
- w_key: bfloat16 [4, 1024, 1024], P(None, None, 'model')
- w_value: bfloat16 [4, 1024, 1024], P(None, None, 'model')
- w_out: bfloat16 [4, 1024, 1024], P(None, 'model')
- w_gate: bfloat16 [4, 1024, 2816], P(None, None, 'model')
- w_up: bfloat16 [4, 1024, 2816], P(None, None, 'model')
- w_down: bfloat16 [4, 2816, 1024], P(None, 'model')
- key_cache: bfloat16 [4, 256, 128, 16, 64], P(None, 'data', None, 'model'), parts along dimension 1
- value_cache: bfloat16 [4, 256, 128, 16, 64], P(None, 'data', None, 'model'), parts along dimension 1
Outputs:
- output 1: bfloat16 [256, 1024], P('data'), parts along dimension 0
- output 2: bfloat16 [4, 256, 128, 16, 64], P(None, 'data', None, 'model'), parts along dimension 1
- output 3: bfloat16 [4, 256, 128, 16, 64], P(None, 'data', None, 'model'), parts along dimension 1
There are 2 independent parts. The reference program is written for one: setup_inputs(seed, part) draws one part's arguments, and reference() takes and returns one part's arrays. A program takes and returns all parts, laid end to end along the dimension named above; an argument that names none is the same for every part.
All inputs are finite; a program needn't handle non-finite values.
Results may differ from the reference program's by a relative error of at most 0.02.
Values are sent between devices in bfloat16 or wider.
A program may use at most 768 MiB of HBM per device.

```python
import math
import jax
import jax.numpy as jnp
from jax import lax

LAYERS = 4
BATCH = 128
CACHE_LEN = 128
MODEL_DIM = 1024
HEADS = 16
KV_HEADS = 16
HEAD_DIM = 64
FF_DIM = 2816
NORM_EPS = 1e-6
ROPE_BASE = 10000.0


def setup_inputs(seed: int = 0, part: int = 0) -> dict:
    root = jax.random.key(seed)
    shared = jax.random.split(root, 9)
    local = jax.random.split(jax.random.fold_in(root, part), 6)
    q_width = HEADS * HEAD_DIM
    kv_width = KV_HEADS * HEAD_DIM
    key_scale = math.sqrt(math.log(CACHE_LEN / 4.0))
    hidden_in = jax.random.normal(local[0], (BATCH, MODEL_DIM), jnp.float32).astype(jnp.bfloat16)
    positions = jax.random.randint(local[1], (BATCH,), 0, CACHE_LEN, dtype=jnp.int32)
    top_row = jax.random.randint(local[2], (), 0, BATCH, dtype=jnp.int32)
    positions = jnp.where(jnp.arange(BATCH) == top_row, CACHE_LEN - 1, positions).astype(jnp.int32)
    norm_attn = jax.random.uniform(shared[0], (LAYERS, MODEL_DIM), jnp.float32, 0.5, 1.5).astype(jnp.bfloat16)
    norm_mlp = jax.random.uniform(shared[1], (LAYERS, MODEL_DIM), jnp.float32, 0.5, 1.5).astype(jnp.bfloat16)
    w_query = (jax.random.normal(shared[2], (LAYERS, MODEL_DIM, q_width), jnp.float32) * MODEL_DIM ** -0.5).astype(jnp.bfloat16)
    w_key = (jax.random.normal(shared[3], (LAYERS, MODEL_DIM, kv_width), jnp.float32) * (key_scale * MODEL_DIM ** -0.5)).astype(jnp.bfloat16)
    w_value = (jax.random.normal(shared[4], (LAYERS, MODEL_DIM, kv_width), jnp.float32) * MODEL_DIM ** -0.5).astype(jnp.bfloat16)
    w_out = (jax.random.normal(shared[5], (LAYERS, q_width, MODEL_DIM), jnp.float32) * q_width ** -0.5).astype(jnp.bfloat16)
    w_gate = (jax.random.normal(shared[6], (LAYERS, MODEL_DIM, FF_DIM), jnp.float32) * MODEL_DIM ** -0.5).astype(jnp.bfloat16)
    w_up = (jax.random.normal(shared[7], (LAYERS, MODEL_DIM, FF_DIM), jnp.float32) * MODEL_DIM ** -0.5).astype(jnp.bfloat16)
    w_down = (jax.random.normal(shared[8], (LAYERS, FF_DIM, MODEL_DIM), jnp.float32) * FF_DIM ** -0.5).astype(jnp.bfloat16)
    cache_shape = (LAYERS, BATCH, CACHE_LEN, KV_HEADS, HEAD_DIM)
    key_cache = (jax.random.normal(local[3], cache_shape, jnp.float32) * key_scale).astype(jnp.bfloat16)
    value_mean = jax.random.normal(local[4], (LAYERS, BATCH, 1, KV_HEADS, HEAD_DIM), jnp.float32)
    value_cache = (value_mean + jax.random.normal(local[5], cache_shape, jnp.float32)).astype(jnp.bfloat16)
    return {"hidden_in": hidden_in, "positions": positions, "norm_attn": norm_attn, "norm_mlp": norm_mlp, "w_query": w_query, "w_key": w_key, "w_value": w_value, "w_out": w_out, "w_gate": w_gate, "w_up": w_up, "w_down": w_down, "key_cache": key_cache, "value_cache": value_cache}


def rms_norm(vals, gain):
    vals_f = vals.astype(jnp.float32)
    inv_rms = lax.rsqrt(jnp.mean(vals_f * vals_f, axis=-1, keepdims=True) + NORM_EPS)
    return (vals_f * inv_rms * gain.astype(jnp.float32)).astype(jnp.bfloat16)


def rope_tables(positions):
    half = HEAD_DIM // 2
    inv_freq = ROPE_BASE ** (-jnp.arange(half, dtype=jnp.float32) / half)
    angles = positions.astype(jnp.float32)[:, None] * inv_freq[None, :]
    return jnp.cos(angles), jnp.sin(angles)


def apply_rope(vals, cos_tab, sin_tab):
    half = HEAD_DIM // 2
    vals_f = vals.astype(jnp.float32)
    first = vals_f[..., :half]
    second = vals_f[..., half:]
    cos_b = cos_tab[:, None, :]
    sin_b = sin_tab[:, None, :]
    return jnp.concatenate([first * cos_b - second * sin_b, second * cos_b + first * sin_b], axis=-1).astype(jnp.bfloat16)


def reference(hidden_in, positions, norm_attn, norm_mlp, w_query, w_key, w_value, w_out, w_gate, w_up, w_down, key_cache, value_cache):
    cos_tab, sin_tab = rope_tables(positions)
    slots = jnp.arange(CACHE_LEN)
    write_row = (slots[None, :] == positions[:, None])[:, :, None, None]
    visible = (slots[None, :] <= positions[:, None])[:, None, None, :]
    group = HEADS // KV_HEADS
    scale = HEAD_DIM ** -0.5

    def layer_step(residual, layer_args):
        g_attn, g_mlp, q_proj, k_proj, v_proj, o_proj, gate_proj, up_proj, down_proj, k_cache, v_cache = layer_args
        hidden = rms_norm(residual, g_attn)
        query = jnp.dot(hidden, q_proj, preferred_element_type=jnp.float32).astype(jnp.bfloat16).reshape(BATCH, HEADS, HEAD_DIM)
        key_new = jnp.dot(hidden, k_proj, preferred_element_type=jnp.float32).astype(jnp.bfloat16).reshape(BATCH, KV_HEADS, HEAD_DIM)
        value_new = jnp.dot(hidden, v_proj, preferred_element_type=jnp.float32).astype(jnp.bfloat16).reshape(BATCH, KV_HEADS, HEAD_DIM)
        query = apply_rope(query, cos_tab, sin_tab)
        key_new = apply_rope(key_new, cos_tab, sin_tab)
        k_cache = jnp.where(write_row, key_new[:, None], k_cache)
        v_cache = jnp.where(write_row, value_new[:, None], v_cache)
        query_g = query.reshape(BATCH, KV_HEADS, group, HEAD_DIM)
        scores = jnp.einsum("bkgd,bskd->bkgs", query_g.astype(jnp.float32), k_cache.astype(jnp.float32)) * scale
        scores = jnp.where(visible, scores, -1e30)
        attn_prob = jax.nn.softmax(scores, axis=-1).astype(jnp.bfloat16)
        attn_val = jnp.einsum("bkgs,bskd->bkgd", attn_prob.astype(jnp.float32), v_cache.astype(jnp.float32)).astype(jnp.bfloat16).reshape(BATCH, HEADS * HEAD_DIM)
        residual = (residual.astype(jnp.float32) + jnp.dot(attn_val, o_proj, preferred_element_type=jnp.float32)).astype(jnp.bfloat16)
        hidden = rms_norm(residual, g_mlp)
        gate_pre = jnp.dot(hidden, gate_proj, preferred_element_type=jnp.float32)
        up_val = jnp.dot(hidden, up_proj, preferred_element_type=jnp.float32)
        act_val = (jax.nn.silu(gate_pre) * up_val).astype(jnp.bfloat16)
        residual = (residual.astype(jnp.float32) + jnp.dot(act_val, down_proj, preferred_element_type=jnp.float32)).astype(jnp.bfloat16)
        return residual, (k_cache, v_cache)

    final, caches = lax.scan(layer_step, hidden_in, (norm_attn, norm_mlp, w_query, w_key, w_value, w_out, w_gate, w_up, w_down, key_cache, value_cache))
    return final, caches[0], caches[1]
```

```python
import functools
import jax
import jax.numpy as jnp
from jax import lax
from jax.experimental import pallas as pl
from jax.experimental.pallas import tpu as pltpu
from jax.sharding import PartitionSpec as P

NORM_EPS = 1e-6
ROPE_BASE = 10000.0
MESH = pl.DeviceIdType.MESH
GROUP = 8
BLOCK = 32
F32 = jnp.float32
BF16 = jnp.bfloat16


def rms_rows(vals_f, gain):
    inv_rms = lax.rsqrt(jnp.mean(vals_f * vals_f, axis=-1, keepdims=True) + NORM_EPS)
    return (vals_f * inv_rms * gain.astype(F32)).astype(BF16)


def rope_tables(positions, head_dim, heads):
    half = head_dim // 2
    inv_freq = ROPE_BASE ** (-jnp.arange(half, dtype=F32) / half)
    angles = positions.astype(F32)[:, None] * inv_freq[None, :]
    cos_tab, sin_tab = jnp.cos(angles), jnp.sin(angles)
    cos_full = jnp.concatenate([cos_tab, cos_tab] * heads, axis=-1)
    sin_full = jnp.concatenate([-sin_tab, sin_tab] * heads, axis=-1)
    return cos_full, sin_full


def attn_kernel(layer, head_dim, scale, first, *refs):
    if first:
        (pos_ref, x_ref, gain_ref, cos_ref, sin_ref, posb_ref, wq_ref, wk_ref, wv_ref, wo_ref, k_ref, v_ref,
         part_ref, ko_ref, vo_ref, q_s, kn_s, vn_s, o_s) = refs
    else:
        (pos_ref, x_ref, gain_ref, cos_ref, sin_ref, posb_ref, wq_ref, wk_ref, wv_ref, wo_ref, k_ref, v_ref, _, _,
         part_ref, ko_ref, vo_ref, q_s, kn_s, vn_s, o_s) = refs
    step = pl.program_id(0)
    tokens, width = q_s.shape[0] // 2, q_s.shape[1]
    half = head_dim // 2
    groups = tokens // GROUP

    def by_head(vals):
        lane = lax.broadcasted_iota(jnp.int32, (groups, GROUP, width), 2)
        vals3 = vals.reshape(groups, GROUP, width)
        low = jnp.where(lane < head_dim, vals3, 0.0)
        high = jnp.where(lane < head_dim, 0.0, vals3)
        return jnp.concatenate([low, high], axis=1).reshape(2 * tokens, width)

    @pl.when(step == 0)
    def _():
        if first:
            hidden = rms_rows(x_ref[...].astype(F32), gain_ref[...])
        else:
            hidden = x_ref[...]
        lane = lax.broadcasted_iota(jnp.int32, (tokens, width), 1)
        lower = lax.rem(lane, head_dim) < half

        def rope(vals):
            turned = jnp.where(lower, pltpu.roll(vals, width - half, 1), pltpu.roll(vals, half, 1))
            return (vals * cos_ref[...] + turned * sin_ref[...]).astype(BF16).astype(F32)

        def project(w_ref):
            return jnp.dot(hidden, w_ref[layer], preferred_element_type=F32).astype(BF16).astype(F32)

        q_s[...] = by_head(rope(project(wq_ref)))
        kn_s[...] = by_head(rope(project(wk_ref)))
        vn_s[...] = by_head(project(wv_ref))

    rows = 2 * GROUP
    row = lax.broadcasted_iota(jnp.int32, (rows, width), 0)
    tok = lax.rem(row, GROUP)
    lane = lax.broadcasted_iota(jnp.int32, (rows, width), 1)
    lane_b = lane.astype(F32).astype(BF16)
    head_low = lax.broadcasted_iota(jnp.int32, (GROUP, width), 1) < head_dim
    per_step = BLOCK // GROUP
    for g in range(per_step):
        base = pl.multiple_of((step * per_step + g) * rows, rows)
        q_f = q_s[pl.ds(base, rows), :]
        kn_f = kn_s[pl.ds(base, rows), :]
        vn_f = vn_s[pl.ds(base, rows), :]
        pos = posb_ref[pl.ds(base, rows), :]
        keys = [k_ref[0, g * GROUP + t] for t in range(GROUP)]
        vals = [v_ref[0, g * GROUP + t] for t in range(GROUP)]
        prod = jnp.dot(q_f.astype(BF16), jnp.concatenate(keys, axis=1), preferred_element_type=F32)
        scores = prod[:, 0:width]
        for t in range(1, GROUP):
            scores = jnp.where(tok == t, prod[:, t * width:(t + 1) * width], scores)
        fresh = jnp.sum(q_f * kn_f, axis=-1, keepdims=True)
        here = lane == pos
        scores = jnp.where(here, fresh, scores) * scale
        scores = jnp.where(lane <= pos, scores, -1e30)
        top = jnp.max(scores, axis=-1, keepdims=True)
        expd = jnp.exp(scores - top)
        prob = (expd / jnp.sum(expd, axis=-1, keepdims=True)).astype(BF16).astype(F32)
        prob_new = jnp.sum(jnp.where(here, prob, 0.0), axis=-1, keepdims=True)
        prob_old = jnp.where(here, 0.0, prob).astype(BF16)
        ctx = lax.dot_general(prob_old, jnp.concatenate(vals, axis=0), (((1,), (1,)), ((), ())), preferred_element_type=F32)
        mixed = ctx[:, 0:width]
        for t in range(1, GROUP):
            mixed = jnp.where(tok == t, ctx[:, t * width:(t + 1) * width], mixed)
        mixed = mixed + prob_new * vn_f
        o_base = pl.multiple_of((step * per_step + g) * GROUP, GROUP)
        o_s[pl.ds(o_base, GROUP), :] = jnp.where(head_low, mixed[:GROUP], mixed[GROUP:])
        hot = jnp.concatenate([jnp.where((tok == t) & here, 1.0, 0.0).astype(BF16) for t in range(GROUP)], axis=1)
        k_col = lax.dot_general(kn_f.astype(BF16), hot, (((0,), (0,)), ((), ())), preferred_element_type=F32)
        v_col = lax.dot_general(vn_f.astype(BF16), hot, (((0,), (0,)), ((), ())), preferred_element_type=F32)
        for t in range(GROUP):
            p_t = pos_ref[(step * per_step + g) * GROUP + t]
            p_b = jnp.full((rows, width), p_t, jnp.int32).astype(F32).astype(BF16)
            mask = jnp.broadcast_to((lane_b == p_b)[None], (width // rows, rows, width))
            for ref, col, old in ((ko_ref, k_col, keys[t]), (vo_ref, v_col, vals[t])):
                new = col[:, t * width:(t + 1) * width].astype(BF16).reshape(width // rows, rows, width)
                ref[0, g * GROUP + t] = jnp.where(mask, new, old.reshape(width // rows, rows, width)).reshape(width, width)

    @pl.when(step == pl.num_programs(0) - 1)
    def _():
        part_ref[...] = jnp.dot(o_s[...].astype(BF16), wo_ref[layer], preferred_element_type=F32).astype(BF16)


def attention(layer, first, pos, x, gain, cos_tab, sin_tab, posb, wq, wk, wv, wo, kc, vc, prev):
    layers, tokens, width, cache_len = kc.shape
    model_dim = x.shape[1]
    head_dim = attention.head_dim
    whole = lambda a: pl.BlockSpec(a.shape, lambda i: (0,) * a.ndim)
    vmem = pl.BlockSpec(memory_space=pltpu.VMEM)
    cache = pl.BlockSpec((1, BLOCK, width, cache_len), lambda i: (layer, i, 0, 0))
    in_specs = [pl.BlockSpec(memory_space=pltpu.SMEM), whole(x), whole(gain), whole(cos_tab), whole(sin_tab), whole(posb),
                vmem, vmem, vmem, vmem, cache, cache]
    args = [pos, x, gain, cos_tab, sin_tab, posb, wq, wk, wv, wo, kc, vc]
    aliases = {}
    if not first:
        in_specs += [pl.BlockSpec(memory_space=pl.ANY)] * 2
        args += list(prev)
        aliases = {12: 1, 13: 2}
    return pl.pallas_call(
        functools.partial(attn_kernel, layer, head_dim, head_dim ** -0.5, first),
        grid=(tokens // BLOCK,),
        in_specs=in_specs,
        out_specs=[pl.BlockSpec((tokens, model_dim), lambda i: (0, 0)), cache, cache],
        out_shape=[jax.ShapeDtypeStruct((tokens, model_dim), BF16), jax.ShapeDtypeStruct(kc.shape, BF16), jax.ShapeDtypeStruct(vc.shape, BF16)],
        scratch_shapes=[pltpu.VMEM((2 * tokens, width), F32), pltpu.VMEM((2 * tokens, width), F32), pltpu.VMEM((2 * tokens, width), F32), pltpu.VMEM((tokens, width), F32)],
        input_output_aliases=aliases,
        compiler_params=pltpu.CompilerParams(dimension_semantics=("arbitrary",), vmem_limit_bytes=28 * 2 ** 20),
        name="attn",
    )(*args)


def mlp_kernel(n, layer, first, last, part_ref, x_ref, gm_ref, ga_ref, wg, wu, wd, h_ref, xo_ref,
               part2, rs_buf, ag_buf, rs_send, rs_recv, ag_send, ag_recv):
    data = lax.axis_index("data")
    me = lax.axis_index("model")
    blk = xo_ref.shape[0]
    peers = [lax.rem(me + d, n) for d in range(1, n)]
    barrier = pltpu.get_barrier_semaphore()
    for peer in peers:
        pl.semaphore_signal(barrier, inc=1, device_id=(data, peer), device_id_type=MESH)
    mine = pl.ds(pl.multiple_of(me * blk, blk), blk)
    order = sorted(range(1, n), key=lambda d: -min(d // 2, n // 2 - d // 2))

    def scatter(src, k):
        copies = []
        for d in order:
            rows = pl.ds(pl.multiple_of(peers[d - 1] * blk, blk), blk)
            copies.append(pltpu.make_async_remote_copy(
                src_ref=src.at[rows], dst_ref=rs_buf.at[k, d - 1], send_sem=rs_send.at[k, d - 1], recv_sem=rs_recv.at[k, d - 1],
                device_id=(data, peers[d - 1]), device_id_type=MESH))
            copies[-1].start()
        return copies

    def reduce(src, k, copies):
        total = src[mine, :].astype(F32)
        for copy in copies:
            copy.wait_recv()
        for d in range(1, n):
            total = total + rs_buf[k, d - 1].astype(F32)
        return total

    def gather(k, value):
        ag_buf[k, mine, :] = value
        copies = []
        for d in order:
            copies.append(pltpu.make_async_remote_copy(
                src_ref=ag_buf.at[k, mine], dst_ref=ag_buf.at[k, mine], send_sem=ag_send.at[k, d - 1], recv_sem=ag_recv.at[k, d - 1],
                device_id=(data, peers[d - 1]), device_id_type=MESH))
            copies[-1].start()
        return copies

    pl.semaphore_wait(barrier, n - 1)
    sent = scatter(part_ref, 0)
    x_old = (x_ref[mine, :] if first else x_ref[...]).astype(F32)
    x_mid = (x_old + reduce(part_ref, 0, sent)).astype(BF16)
    sent2 = gather(0, rms_rows(x_mid.astype(F32), gm_ref[...]))
    for copy in sent2:
        copy.wait_recv()
    hidden = ag_buf[0]
    nt = (((1,), (1,)), ((), ()))
    gate = lax.dot_general(hidden, wg[layer], nt, preferred_element_type=F32)
    up = lax.dot_general(hidden, wu[layer], nt, preferred_element_type=F32)
    act = (jax.nn.silu(gate) * up).astype(BF16)
    part2[...] = jnp.dot(act, wd[layer], preferred_element_type=F32).astype(BF16)
    sent3 = scatter(part2, 1)
    x_new = (x_mid.astype(F32) + reduce(part2, 1, sent3)).astype(BF16)
    xo_ref[...] = x_new
    sent4 = gather(1, x_new if last else rms_rows(x_new.astype(F32), ga_ref[...]))
    for copy in sent4:
        copy.wait_recv()
    h_ref[...] = ag_buf[1]
    for copies in (sent, sent2, sent3, sent4):
        for copy in copies:
            copy.wait_send()


def mlp(n, layer, layers, part, x, gm, ga, wg, wu, wd):
    tokens, model_dim = part.shape
    blk = tokens // n
    vmem = pl.BlockSpec(memory_space=pltpu.VMEM)
    return pl.pallas_call(
        functools.partial(mlp_kernel, n, layer, layer == 0, layer == layers - 1),
        in_specs=[vmem] * 7,
        out_specs=[vmem, vmem],
        out_shape=[jax.ShapeDtypeStruct((tokens, model_dim), BF16), jax.ShapeDtypeStruct((blk, model_dim), BF16)],
        scratch_shapes=[pltpu.VMEM((tokens, model_dim), BF16), pltpu.VMEM((2, n - 1, blk, model_dim), BF16), pltpu.VMEM((2, tokens, model_dim), BF16),
                        pltpu.SemaphoreType.DMA((2, n - 1)), pltpu.SemaphoreType.DMA((2, n - 1)),
                        pltpu.SemaphoreType.DMA((2, n - 1)), pltpu.SemaphoreType.DMA((2, n - 1))],
        compiler_params=pltpu.CompilerParams(collective_id=layer, has_side_effects=True, vmem_limit_bytes=20 * 2 ** 20),
        name="mlp",
    )(part, x, gm, ga, wg, wu, wd)


def solution(mesh):
    n = mesh.shape["model"]

    def local_step(hidden_in, positions, norm_attn, norm_mlp, w_query, w_key, w_value, w_out, w_gate, w_up, w_down, key_cache, value_cache):
        layers, tokens, cache_len, heads, head_dim = key_cache.shape
        attention.head_dim = head_dim
        width = heads * head_dim
        cos_tab, sin_tab = rope_tables(positions, head_dim, heads)
        posb = jnp.broadcast_to(positions.reshape(tokens // GROUP, 1, GROUP, 1), (tokens // GROUP, heads, GROUP, cache_len)).reshape(heads * tokens, cache_len)
        fold = lambda c: jnp.transpose(c, (0, 1, 3, 4, 2)).reshape(layers, tokens, width, cache_len)
        unfold = lambda c: jnp.transpose(c.reshape(layers, tokens, heads, head_dim, cache_len), (0, 1, 4, 2, 3))
        kc, vc = (pltpu.with_memory_space_constraint(fold(c), pltpu.HBM) for c in (key_cache, value_cache))
        wg, wu = jnp.swapaxes(w_gate, 1, 2), jnp.swapaxes(w_up, 1, 2)
        hidden, x_rows, prev = hidden_in, hidden_in, None
        for layer in range(layers):
            part, k_new, v_new = attention(layer, layer == 0, positions, hidden, norm_attn[layer:layer + 1], cos_tab, sin_tab, posb, w_query, w_key, w_value, w_out, kc, vc, prev)
            prev = (k_new, v_new)
            nxt = min(layer + 1, layers - 1)
            hidden, x_rows = mlp(n, layer, layers, part, x_rows, norm_mlp[layer:layer + 1], norm_attn[nxt:nxt + 1], wg, wu, w_down)
        return hidden, unfold(prev[0]), unfold(prev[1])

    row_spec = P("data", None)
    col_spec = P(None, None, "model")
    split_spec = P(None, "model", None)
    cache_spec = P(None, "data", None, "model", None)
    in_specs = (row_spec, P("data"), P(None, None), P(None, None), col_spec, col_spec, col_spec, split_spec, col_spec, col_spec, split_spec, cache_spec, cache_spec)
    out_specs = (row_spec, cache_spec, cache_spec)
    return jax.shard_map(local_step, mesh=mesh, in_specs=in_specs, out_specs=out_specs, check_vma=False)
```

```python
import functools
import numpy as np
import jax
import jax.numpy as jnp
from jax import lax
from jax.experimental import pallas as pl
from jax.experimental.pallas import tpu as pltpu
from jax.sharding import PartitionSpec as P

NORM_EPS = 1e-6
ROPE_BASE = 10000.0
MESH = pl.DeviceIdType.MESH
GROUP = 8
BLOCK = 32
F32 = jnp.float32
BF16 = jnp.bfloat16


def rms_rows(vals_f, gain):
    inv_rms = lax.rsqrt(jnp.mean(vals_f * vals_f, axis=-1, keepdims=True) + NORM_EPS)
    return (vals_f * inv_rms * gain.astype(F32)).astype(BF16)


def rope_freqs(head_dim, heads):
    half = head_dim // 2
    inv_freq = ROPE_BASE ** (-np.arange(half, dtype=np.float32) / np.float32(half))
    return np.tile(inv_freq.astype(np.float32), 2 * heads)[None, :]


def attn_kernel(layer, head_dim, scale, first, *refs):
    if first:
        (pos_ref, freq_ref, x_ref, gain_ref, wq_ref, wk_ref, wv_ref, wo_ref, k_ref, v_ref,
         part_ref, ko_ref, vo_ref, cos_ref, sin_ref, posr_ref, q_s, kn_s, vn_s, o_s) = refs
    else:
        (cos_ref, sin_ref, posr_ref, x_ref, wq_ref, wk_ref, wv_ref, wo_ref, k_ref, v_ref, _, _,
         part_ref, ko_ref, vo_ref, q_s, kn_s, vn_s, o_s) = refs
    step = pl.program_id(0)
    tokens, width = q_s.shape[0] // 2, q_s.shape[1]
    half = head_dim // 2
    groups = tokens // GROUP

    def by_head(vals):
        lane = lax.broadcasted_iota(jnp.int32, (groups, GROUP, width), 2)
        vals3 = vals.reshape(groups, GROUP, width)
        low = jnp.where(lane < head_dim, vals3, 0.0)
        high = jnp.where(lane < head_dim, 0.0, vals3)
        return jnp.concatenate([low, high], axis=1).reshape(2 * tokens, width)

    @pl.when(step == 0)
    def _():
        lane = lax.broadcasted_iota(jnp.int32, (tokens, width), 1)
        lower = lax.rem(lane, head_dim) < half
        if first:
            posr = jnp.transpose(jnp.broadcast_to(pos_ref[...].astype(F32), (width, tokens)))
            posr_ref[...] = posr
            angle = posr * freq_ref[...]
            cos_ref[...] = jnp.cos(angle)
            sin_ref[...] = jnp.where(lower, -1.0, 1.0) * jnp.sin(angle)
            hidden = rms_rows(x_ref[...].astype(F32), gain_ref[layer:layer + 1, :])
        else:
            hidden = x_ref[...]

        def rope(vals):
            turned = jnp.where(lower, pltpu.roll(vals, width - half, 1), pltpu.roll(vals, half, 1))
            return (vals * cos_ref[...] + turned * sin_ref[...]).astype(BF16).astype(F32)

        def project(w_ref):
            return jnp.dot(hidden, w_ref[0 if first else layer], preferred_element_type=F32).astype(BF16).astype(F32)

        q_s[...] = by_head(rope(project(wq_ref)))
        kn_s[...] = by_head(rope(project(wk_ref)))
        vn_s[...] = by_head(project(wv_ref))

    rows = 2 * GROUP
    row = lax.broadcasted_iota(jnp.int32, (rows, width), 0)
    tok = lax.rem(row, GROUP)
    lane = lax.broadcasted_iota(jnp.int32, (rows, width), 1).astype(F32)
    lane_b = lane.astype(BF16)
    head_low = lax.broadcasted_iota(jnp.int32, (GROUP, width), 1) < head_dim
    per_step = BLOCK // GROUP
    for g in range(per_step):
        base = pl.multiple_of((step * per_step + g) * rows, rows)
        tok_base = pl.multiple_of((step * per_step + g) * GROUP, GROUP)
        q_f = q_s[pl.ds(base, rows), :]
        kn_f = kn_s[pl.ds(base, rows), :]
        vn_f = vn_s[pl.ds(base, rows), :]
        pos8 = posr_ref[pl.ds(tok_base, GROUP), :]
        pos = jnp.concatenate([pos8, pos8], axis=0)
        if first:
            keys = [k_ref[0, g * GROUP + t] for t in range(GROUP)]
            vals = [v_ref[0, g * GROUP + t] for t in range(GROUP)]
        else:
            keys = [k_ref[tok_base + t] for t in range(GROUP)]
            vals = [v_ref[tok_base + t] for t in range(GROUP)]
        prod = jnp.dot(q_f.astype(BF16), jnp.concatenate(keys, axis=1), preferred_element_type=F32)
        scores = prod[:, 0:width]
        for t in range(1, GROUP):
            scores = jnp.where(tok == t, prod[:, t * width:(t + 1) * width], scores)
        fresh = jnp.sum(q_f * kn_f, axis=-1, keepdims=True)
        here = lane == pos
        scores = jnp.where(here, fresh, scores) * scale
        scores = jnp.where(lane <= pos, scores, -1e30)
        top = jnp.max(scores, axis=-1, keepdims=True)
        expd = jnp.exp(scores - top)
        prob = (expd / jnp.sum(expd, axis=-1, keepdims=True)).astype(BF16).astype(F32)
        prob_new = jnp.sum(jnp.where(here, prob, 0.0), axis=-1, keepdims=True)
        prob_old = jnp.where(here, 0.0, prob).astype(BF16)
        ctx = lax.dot_general(prob_old, jnp.concatenate(vals, axis=0), (((1,), (1,)), ((), ())), preferred_element_type=F32)
        mixed = ctx[:, 0:width]
        for t in range(1, GROUP):
            mixed = jnp.where(tok == t, ctx[:, t * width:(t + 1) * width], mixed)
        mixed = mixed + prob_new * vn_f
        o_s[pl.ds(tok_base, GROUP), :] = jnp.where(head_low, mixed[:GROUP], mixed[GROUP:])
        hot = jnp.concatenate([jnp.where((tok == t) & here, 1.0, 0.0).astype(BF16) for t in range(GROUP)], axis=1)
        k_col = lax.dot_general(kn_f.astype(BF16), hot, (((0,), (0,)), ((), ())), preferred_element_type=F32)
        v_col = lax.dot_general(vn_f.astype(BF16), hot, (((0,), (0,)), ((), ())), preferred_element_type=F32)
        for t in range(GROUP):
            p_b = jnp.broadcast_to(posr_ref[pl.ds(tok_base + t, 1), :], (rows, width)).astype(BF16)
            mask = jnp.broadcast_to((lane_b == p_b)[None], (width // rows, rows, width))
            for ref, col, old in ((ko_ref, k_col, keys[t]), (vo_ref, v_col, vals[t])):
                new = col[:, t * width:(t + 1) * width].astype(BF16).reshape(width // rows, rows, width)
                ref[0, g * GROUP + t] = jnp.where(mask, new, old.reshape(width // rows, rows, width)).reshape(width, width)

    @pl.when(step == pl.num_programs(0) - 1)
    def _():
        part_ref[...] = jnp.dot(o_s[...].astype(BF16), wo_ref[0 if first else layer], preferred_element_type=F32).astype(BF16)


def attention(layer, head_dim, lead, x, weights, caches, shape, prev):
    first = layer == 0
    layers, tokens, width, cache_len = shape
    model_dim = x.shape[1]
    vmem = pl.BlockSpec(memory_space=pltpu.VMEM)
    whole = lambda a: pl.BlockSpec(a.shape, lambda i: (0,) * a.ndim)
    of_layer = lambda a: pl.BlockSpec((1,) + a.shape[1:], lambda i: (layer,) + (0,) * (a.ndim - 1))
    cache = pl.BlockSpec((1, BLOCK, width, cache_len), lambda i: (layer, i, 0, 0))
    table = jax.ShapeDtypeStruct((tokens, width), F32)
    out_specs = [pl.BlockSpec((tokens, model_dim), lambda i: (0, 0)), cache, cache]
    out_shape = [jax.ShapeDtypeStruct((tokens, model_dim), BF16), jax.ShapeDtypeStruct(shape, BF16), jax.ShapeDtypeStruct(shape, BF16)]
    aliases = {}
    if first:
        pos, freq, gain = lead
        in_specs = [whole(pos), whole(freq), whole(x), whole(gain)] + [of_layer(w) for w in weights] + [cache, cache]
        args = [pos, freq, x, gain, *weights, *caches]
        out_specs += [pl.BlockSpec((tokens, width), lambda i: (0, 0))] * 3
        out_shape += [table] * 3
    else:
        in_specs = [vmem] * 10 + [pl.BlockSpec(memory_space=pl.ANY)] * 2
        args = [*lead, x, *weights, *caches, *prev]
        aliases = {10: 1, 11: 2}
    return pl.pallas_call(
        functools.partial(attn_kernel, layer, head_dim, head_dim ** -0.5, first),
        grid=(tokens // BLOCK,),
        in_specs=in_specs,
        out_specs=out_specs,
        out_shape=out_shape,
        scratch_shapes=[pltpu.VMEM((2 * tokens, width), F32), pltpu.VMEM((2 * tokens, width), F32), pltpu.VMEM((2 * tokens, width), F32), pltpu.VMEM((tokens, width), F32)],
        input_output_aliases=aliases,
        compiler_params=pltpu.CompilerParams(dimension_semantics=("arbitrary",), vmem_limit_bytes=28 * 2 ** 20),
        name="attn",
    )(*args)


def mlp_kernel(n, layer, first, last, *refs):
    if last:
        part_ref, x_ref, gm_ref, ga_ref, wg, wu, wd, h_ref, xo_ref, part2, rs_buf, ag_buf, rs_send, rs_recv, ag_send, ag_recv = refs
        loads = []
    else:
        (part_ref, x_ref, gm_ref, ga_ref, wg, wu, wd, kc_ref, vc_ref, h_ref, xo_ref, k_out, v_out,
         part2, rs_buf, ag_buf, rs_send, rs_recv, ag_send, ag_recv, load_sem) = refs
        loads = [pltpu.make_async_copy(src.at[layer + 1], dst, load_sem.at[i]) for i, (src, dst) in enumerate(((kc_ref, k_out), (vc_ref, v_out)))]
    data = lax.axis_index("data")
    me = lax.axis_index("model")
    blk = xo_ref.shape[0]
    peers = [lax.rem(me + d, n) for d in range(1, n)]
    barrier = pltpu.get_barrier_semaphore()
    for peer in peers:
        pl.semaphore_signal(barrier, inc=1, device_id=(data, peer), device_id_type=MESH)
    mine = pl.ds(pl.multiple_of(me * blk, blk), blk)
    order = sorted(range(1, n), key=lambda d: -min(d // 2, n // 2 - d // 2))

    def scatter(src, k):
        copies = []
        for d in order:
            rows = pl.ds(pl.multiple_of(peers[d - 1] * blk, blk), blk)
            copies.append(pltpu.make_async_remote_copy(
                src_ref=src.at[rows], dst_ref=rs_buf.at[k, d - 1], send_sem=rs_send.at[k, d - 1], recv_sem=rs_recv.at[k, d - 1],
                device_id=(data, peers[d - 1]), device_id_type=MESH))
            copies[-1].start()
        return copies

    def reduce(src, k, copies):
        total = src[mine, :].astype(F32)
        for copy in copies:
            copy.wait_recv()
        for d in range(1, n):
            total = total + rs_buf[k, d - 1].astype(F32)
        return total

    def gather(k, value):
        ag_buf[k, mine, :] = value
        copies = []
        for d in order:
            copies.append(pltpu.make_async_remote_copy(
                src_ref=ag_buf.at[k, mine], dst_ref=ag_buf.at[k, mine], send_sem=ag_send.at[k, d - 1], recv_sem=ag_recv.at[k, d - 1],
                device_id=(data, peers[d - 1]), device_id_type=MESH))
            copies[-1].start()
        return copies

    for load in loads:
        load.start()
    pl.semaphore_wait(barrier, n - 1)
    sent = scatter(part_ref, 0)
    x_old = (x_ref[mine, :] if first else x_ref[...]).astype(F32)
    x_mid = (x_old + reduce(part_ref, 0, sent)).astype(BF16)
    sent2 = gather(0, rms_rows(x_mid.astype(F32), gm_ref[layer:layer + 1, :]))
    for copy in sent2:
        copy.wait_recv()
    hidden = ag_buf[0]
    nt = (((1,), (1,)), ((), ()))
    gate = lax.dot_general(hidden, wg[layer], nt, preferred_element_type=F32)
    up = lax.dot_general(hidden, wu[layer], nt, preferred_element_type=F32)
    act = (jax.nn.silu(gate) * up).astype(BF16)
    part2[...] = jnp.dot(act, wd[layer], preferred_element_type=F32).astype(BF16)
    sent3 = scatter(part2, 1)
    x_new = (x_mid.astype(F32) + reduce(part2, 1, sent3)).astype(BF16)
    xo_ref[...] = x_new
    sent4 = gather(1, x_new if last else rms_rows(x_new.astype(F32), ga_ref[layer + 1:layer + 2, :]))
    for copy in sent4:
        copy.wait_recv()
    h_ref[...] = ag_buf[1]
    for copies in (sent, sent2, sent3, sent4):
        for copy in copies:
            copy.wait_send()
    for load in loads:
        load.wait()


def mlp(n, layer, part, x, gm, ga, wg, wu, wd, kc, vc):
    tokens, model_dim = part.shape
    blk = tokens // n
    last = layer == kc.shape[0] - 1
    vmem = pl.BlockSpec(memory_space=pltpu.VMEM)
    ahead = [] if last else [kc, vc]
    return pl.pallas_call(
        functools.partial(mlp_kernel, n, layer, layer == 0, last),
        in_specs=[vmem] * 7 + [pl.BlockSpec(memory_space=pl.ANY)] * len(ahead),
        out_specs=[vmem] * (2 + len(ahead)),
        out_shape=[jax.ShapeDtypeStruct((tokens, model_dim), BF16), jax.ShapeDtypeStruct((blk, model_dim), BF16)] + [pltpu.VMEM(c.shape[1:], BF16) for c in ahead],
        scratch_shapes=[pltpu.VMEM((tokens, model_dim), BF16), pltpu.VMEM((2, n - 1, blk, model_dim), BF16), pltpu.VMEM((2, tokens, model_dim), BF16),
                        pltpu.SemaphoreType.DMA((2, n - 1)), pltpu.SemaphoreType.DMA((2, n - 1)),
                        pltpu.SemaphoreType.DMA((2, n - 1)), pltpu.SemaphoreType.DMA((2, n - 1))] + ([] if last else [pltpu.SemaphoreType.DMA((2,))]),
        compiler_params=pltpu.CompilerParams(collective_id=layer, has_side_effects=True, vmem_limit_bytes=20 * 2 ** 20),
        name="mlp",
    )(part, x, gm, ga, wg, wu, wd, *ahead)


def solution(mesh):
    n = mesh.shape["model"]

    def local_step(hidden_in, positions, norm_attn, norm_mlp, w_query, w_key, w_value, w_out, w_gate, w_up, w_down, key_cache, value_cache):
        layers, tokens, cache_len, heads, head_dim = key_cache.shape
        shape = (layers, tokens, heads * head_dim, cache_len)
        in_hbm = lambda a: pltpu.with_memory_space_constraint(a, pltpu.HBM)
        unfold = lambda c: jnp.transpose(c.reshape(layers, tokens, heads, head_dim, cache_len), (0, 1, 4, 2, 3))
        kc, vc = (in_hbm(jnp.transpose(c, (0, 1, 3, 4, 2)).reshape(shape)) for c in (key_cache, value_cache))
        wg, wu = jnp.swapaxes(w_gate, 1, 2), jnp.swapaxes(w_up, 1, 2)
        weights = (w_query, w_key, w_value, w_out)
        freq = jnp.asarray(rope_freqs(head_dim, heads))
        part, k_new, v_new, *tables = attention(0, head_dim, (in_hbm(positions.reshape(1, tokens)), freq, in_hbm(norm_attn)), in_hbm(hidden_in), [in_hbm(w) for w in weights], (kc, vc), shape, None)
        x_rows = hidden_in
        for layer in range(layers):
            hidden, x_rows, *caches = mlp(n, layer, part, x_rows, norm_mlp, norm_attn, wg, wu, w_down, kc, vc)
            if layer + 1 < layers:
                part, k_new, v_new = attention(layer + 1, head_dim, tables, hidden, weights, caches, shape, (k_new, v_new))
        return hidden, unfold(k_new), unfold(v_new)

    row_spec = P("data", None)
    col_spec = P(None, None, "model")
    split_spec = P(None, "model", None)
    cache_spec = P(None, "data", None, "model", None)
    in_specs = (row_spec, P("data"), P(None, None), P(None, None), col_spec, col_spec, col_spec, split_spec, col_spec, col_spec, split_spec, cache_spec, cache_spec)
    out_specs = (row_spec, cache_spec, cache_spec)
    return jax.shard_map(local_step, mesh=mesh, in_specs=in_specs, out_specs=out_specs, check_vma=False)
```
